128 devices in a mesh: blk: 128 (over y, x, z, core).
Axes of the slice: x: 4, y: 4, z: 4, core: 2. Of those that a mesh axis runs over, the one named last changes fastest.
Arguments:
- node_latent: bfloat16 [524288, 128], P('blk'), may hold values from -16 to 16
- edge_latent: bfloat16 [3145728, 128], P('blk'), may hold values from -6 to 6
- edge_ends: int32 [2, 3145728], P(None, 'blk'), may hold values from 0 to 5631, as said below
- edge_owned: int32 [3145728], P('blk'), may hold values from 0 to 1, as said below
- send_index: int32 [128, 6, 256], P('blk'), may hold values from 0 to 4095, as said below
- edge_w1: bfloat16 [2, 384, 128], replicated, may hold values from -0.3125 to 0.3125
- edge_b1: float32 [2, 128], replicated, may hold values from -3 to 3
- edge_w2: bfloat16 [2, 128, 128], replicated, may hold values from -0.5 to 0.5
- edge_gain: float32 [2, 128], replicated, may hold values from 0.5 to 1.5
- edge_shift: float32 [2, 128], replicated, may hold values from -2 to 2
- node_w1: bfloat16 [2, 256, 128], replicated, may hold values from -0.375 to 0.375
- node_b1: float32 [2, 128], replicated, may hold values from -3 to 3
- node_w2: bfloat16 [2, 128, 128], replicated, may hold values from -0.5 to 0.5
- node_gain: float32 [2, 128], replicated, may hold values from 0.5 to 1.5
- node_shift: float32 [2, 128], replicated, may hold values from -2 to 2
Outputs:
- node_out: bfloat16 [524288, 128], P('blk')
- edge_out: bfloat16 [3145728, 128], P('blk')
The draws below stay inside these ranges and needn't reach their ends.
Inputs may be any that keep to these rules, and one draw needn't show every extreme that they name: edge_ends[0] holds each slot's sender, edge_ends[1] its receiver, as entries of the block's extended node list. Slot s of a block lies in tile t = s // 128; each of its ends is either an own node from (t // 6) * 128 to (t // 6 + 1) * 128 - 1 or a halo entry from 4096 + (t % 6) * 256 to 4096 + (t % 6 + 1) * 256 - 1; at most one end of a slot is a halo entry. `edge_owned`: in each block the slots with 1 come first; every block has at least 15360 of them. send_index[b, k] lists 256 distinct nodes of block b.
All inputs are finite; a program needn't handle non-finite values.
Results may differ from the reference program's by a relative error of at most 0.0085.
Values may be sent and summed in bfloat16 or wider, within the bound.
A program may use at most 128 MiB of HBM per device.

```python
import jax
import jax.numpy as jnp
from jax import lax

LATENT = 128
NODE_DEV = 4096
HALO = 256
LAYERS = 2
FACES = 6
GX = 4
GY = 4
EDGE_TILE = 128
EDGE_DEV = 24576
EDGES = 3145728
N_BLK = 128


def draw_node_latent(key, part):
    total_rows = NODE_DEV * N_BLK
    position = jnp.arange(total_rows, dtype=jnp.float32)[:, None] / (total_rows - 1)
    values = jnp.clip(jax.random.normal(key, (total_rows, LATENT), jnp.float32), -5.0, 5.0)
    scales = 1.0 + 2.0 * position
    return (values * scales).astype(jnp.bfloat16)


def draw_edge_ends(key, part):
    total_slots = EDGE_DEV * N_BLK
    subkeys = jax.random.split(jax.random.fold_in(key, 11), 4)
    slot = jnp.arange(total_slots, dtype=jnp.int32) % EDGE_DEV
    tile_id = slot // EDGE_TILE
    own_base = tile_id // FACES * EDGE_TILE
    halo_base = NODE_DEV + tile_id % FACES * HALO
    categories = jax.random.randint(subkeys[0], (total_slots,), 0, 8)
    first_local = jax.random.randint(subkeys[1], (total_slots,), 0, EDGE_TILE)
    step_by = jax.random.randint(subkeys[2], (total_slots,), 1, EDGE_TILE)
    second_local = (first_local + step_by) % EDGE_TILE
    remote = halo_base + jax.random.randint(subkeys[3], (total_slots,), 0, HALO)
    senders = jnp.where(categories < 2, remote, own_base + first_local)
    receivers = jnp.where((categories >= 2) & (categories < 4), remote, own_base + second_local)
    return jnp.stack([senders, receivers]).astype(jnp.int32)


def draw_edge_owned(key, part):
    subkeys = jax.random.split(jax.random.fold_in(key, 17), 2)
    counts = jax.random.randint(subkeys[0], (N_BLK,), EDGE_DEV * 5 // 8, EDGE_DEV + 1)
    fullest = jax.random.randint(subkeys[1], (), 0, N_BLK)
    counts = jnp.where(jnp.arange(N_BLK) == fullest, EDGE_DEV, counts)
    slots = jnp.arange(EDGE_DEV)[None, :] < counts[:, None]
    return slots.astype(jnp.int32).reshape(-1)


def pick_rows(subkey):
    return jax.random.permutation(subkey, NODE_DEV)[:HALO]


def draw_send_index(key, part):
    subkeys = jax.random.split(jax.random.fold_in(key, 23), N_BLK * FACES)
    picked = jax.vmap(pick_rows)(subkeys)
    return picked.reshape(N_BLK, FACES, HALO).astype(jnp.int32)


def steps_of(rng, extent, cuts, least, high):
    loudness, own = 1.0, jax.random.fold_in(rng, 6)
    for dim, parts in cuts:
        steps = jnp.exp(jax.random.uniform(jax.random.fold_in(own, dim), (parts,), jnp.float32, least / len(cuts), high / len(cuts)))
        loudness = loudness * jnp.repeat(steps, extent[dim] // parts).reshape([-1 if axis == dim else 1 for axis in range(len(extent))])
    return loudness


def noise(key, shape, scale, limit, cuts=(), kind=jnp.bfloat16):
    level = steps_of(key, shape, cuts, -0.22, 0.18) if cuts else 1.0
    values = jax.random.normal(key, shape, jnp.float32) * scale * level
    return jnp.minimum(jnp.maximum(values, -limit), limit).astype(kind)


def setup_inputs(seed: int = 0) -> dict:
    arg_keys = jax.random.split(jax.random.key(seed), 16)
    node_latent = draw_node_latent(jax.random.fold_in(arg_keys[15], 71), 0)
    edge_latent = noise(arg_keys[1], (EDGES, LATENT), 1.0, 6.0, ((0, 128),))
    edge_ends = draw_edge_ends(jax.random.fold_in(arg_keys[15], 71), 0)
    edge_owned = draw_edge_owned(jax.random.fold_in(arg_keys[15], 71), 0)
    send_index = draw_send_index(jax.random.fold_in(arg_keys[15], 71), 0)
    edge_w1 = noise(arg_keys[5], (LAYERS, 3 * LATENT, LATENT), (3 * LATENT) ** -0.5, 0.3125)
    edge_b1 = noise(arg_keys[6], (LAYERS, LATENT), 0.5, 3.0, (), jnp.float32)
    edge_w2 = noise(arg_keys[7], (LAYERS, LATENT, LATENT), LATENT ** -0.5, 0.5)
    edge_gain = jnp.clip(1.0 + 0.1 * jax.random.normal(arg_keys[8], (LAYERS, LATENT), jnp.float32), 0.5, 1.5)
    edge_shift = noise(arg_keys[9], (LAYERS, LATENT), 0.3, 2.0, (), jnp.float32)
    node_w1 = noise(arg_keys[10], (LAYERS, 2 * LATENT, LATENT), (2 * LATENT) ** -0.5, 0.375)
    node_b1 = noise(arg_keys[11], (LAYERS, LATENT), 0.5, 3.0, (), jnp.float32)
    node_w2 = noise(arg_keys[12], (LAYERS, LATENT, LATENT), LATENT ** -0.5, 0.5)
    node_gain = jnp.clip(1.0 + 0.1 * jax.random.normal(arg_keys[13], (LAYERS, LATENT), jnp.float32), 0.5, 1.5)
    node_shift = noise(arg_keys[14], (LAYERS, LATENT), 0.3, 2.0, (), jnp.float32)
    return {"node_latent": node_latent, "edge_latent": edge_latent, "edge_ends": edge_ends, "edge_owned": edge_owned, "send_index": send_index, "edge_w1": edge_w1, "edge_b1": edge_b1, "edge_w2": edge_w2, "edge_gain": edge_gain, "edge_shift": edge_shift, "node_w1": node_w1, "node_b1": node_b1, "node_w2": node_w2, "node_gain": node_gain, "node_shift": node_shift}


def row_norm(mixed):
    centre = mixed - lax.optimization_barrier(jnp.mean(mixed, axis=1, keepdims=True))
    spread = lax.optimization_barrier(jnp.mean(centre * centre, axis=1, keepdims=True))
    return centre * lax.rsqrt(spread + 1e-05)

def reference(node_latent, edge_latent, edge_ends, edge_owned, send_index, edge_w1, edge_b1, edge_w2, edge_gain, edge_shift, node_w1, node_b1, node_w2, node_gain, node_shift):
    offsets = jnp.array([1, -1, GX, -GX, GX * GY, -GX * GY], dtype=jnp.int32)
    blocks = jnp.arange(N_BLK, dtype=jnp.int32)
    source = jnp.mod(blocks[:, None] - offsets[None, :], N_BLK).astype(jnp.int32)
    face_ids = jnp.arange(FACES, dtype=jnp.int32)[None, :]
    halo_nodes = source[:, :, None] * NODE_DEV + send_index[source, face_ids]
    own_nodes = blocks[:, None] * NODE_DEV + jnp.arange(NODE_DEV, dtype=jnp.int32)[None, :]
    lookup = jnp.concatenate([own_nodes, halo_nodes.reshape(N_BLK, FACES * HALO)], axis=1).astype(jnp.int32)
    ends = edge_ends.reshape(2, N_BLK, EDGE_DEV)
    senders = jnp.take_along_axis(lookup, ends[0], axis=1)
    receivers = jnp.take_along_axis(lookup, ends[1], axis=1)
    owned = edge_owned.reshape(N_BLK, EDGE_DEV).astype(jnp.float32)
    latents = node_latent
    edge_state = edge_latent.reshape(N_BLK, EDGE_DEV, LATENT)
    for layer_id in range(LAYERS):

        def edge_block(totals, item, latents=latents, layer_id=layer_id):
            block_edges, block_send, block_recv, block_owned = item
            joined = jnp.concatenate([block_edges, latents[block_send], latents[block_recv]], axis=1)
            hidden = jax.nn.relu(jnp.dot(joined, edge_w1[layer_id], preferred_element_type=jnp.float32) + edge_b1[layer_id]).astype(jnp.bfloat16)
            mixed = jnp.dot(hidden, edge_w2[layer_id], preferred_element_type=jnp.float32)
            normed = edge_gain[layer_id] * row_norm(mixed) + edge_shift[layer_id]
            edges_new = (block_edges.astype(jnp.float32) + block_owned[:, None] * normed).astype(jnp.bfloat16)
            totals = totals.at[block_recv].add(block_owned[:, None] * edges_new.astype(jnp.float32))
            return (totals, edges_new)
        start = jnp.zeros((N_BLK * NODE_DEV, LATENT), jnp.float32)
        totals, edge_state = lax.scan(edge_block, start, (edge_state, senders, receivers, owned))
        aggregate = totals.astype(jnp.bfloat16)
        node_in = jnp.concatenate([latents, aggregate], axis=1)
        node_hidden = jax.nn.relu(jnp.dot(node_in, node_w1[layer_id], preferred_element_type=jnp.float32) + node_b1[layer_id]).astype(jnp.bfloat16)
        update = jnp.dot(node_hidden, node_w2[layer_id], preferred_element_type=jnp.float32)
        centre_mean = lax.optimization_barrier(jnp.mean(update, axis=0))
        deviation = update - centre_mean
        variance = lax.optimization_barrier(jnp.mean(deviation * deviation, axis=0))
        latents = (latents.astype(jnp.float32) + node_gain[layer_id] * deviation * lax.rsqrt(variance + 1e-05) + node_shift[layer_id]).astype(jnp.bfloat16)
    return (latents, edge_state.reshape(N_BLK * EDGE_DEV, LATENT))
```

```python
import functools

import jax
import jax.numpy as jnp
from jax import lax
from jax.experimental import pallas as pl
from jax.experimental.pallas import tpu as pltpu
from jax.sharding import PartitionSpec as P

MESH = pl.DeviceIdType.MESH
F32 = jnp.float32
BF16 = jnp.bfloat16
LAYERS = 2
FACES = 6
PAIRS = 3
T = 128
H = 256
GB = 4
REF = 16
ROWS = 512


def dot(a, b):
    return jnp.dot(a, b, preferred_element_type=F32)


def dot_t(a, b):
    return lax.dot_general(a, b, (((1,), (1,)), ((), ())), preferred_element_type=F32)


def columns(row):
    return jnp.broadcast_to(row, (T, T)).T


def hot(index, rows):
    lanes = index.shape[1]
    code = jnp.broadcast_to(index, (16, lanes)).astype(jnp.int16)
    line = lax.broadcasted_iota(jnp.int32, (rows, lanes), 0).astype(jnp.int16)
    same = line.reshape(rows // 16, 16, lanes) == code[None]
    return jnp.where(same, jnp.ones((), BF16), jnp.zeros((), BF16)).reshape(rows, lanes)


def kernel(
    n_dev,
    groups,
    node_ref,
    edge_hbm,
    ends_ref,
    owned_ref,
    send_smem,
    send_ref,
    ew1,
    eb1,
    ew2,
    eg,
    es,
    nw1,
    nb1,
    nw2,
    ng,
    ns,
    node_out,
    edge_out,
    a_buf,
    b_buf,
    hb,
    rowsrc,
    agg,
    tab,
    htab,
    hid,
    ohr,
    ohh,
    hsum,
    stage,
    tx0,
    tx1,
    rx0,
    rx1,
    ret_tx,
    ret_rx,
    w_t,
    cols,
    st_tx,
    st_a,
    st_b,
    in_sem,
    out_sem,
    h_send,
    h_recv,
    r_send,
    r_recv,
    a_send,
    a_recv,
    b_send,
    b_recv,
):
    me = lax.axis_index("blk")
    nodes = groups * T
    blocks = groups // GB
    low, high = lax.rem(me, 8), lax.div(me, 8)
    n_high = n_dev // 8
    offsets = (1, n_dev - 1, 4, n_dev - 4, 16, n_dev - 16)

    def ahead(distance):
        return lax.rem(me + distance, n_dev)

    def partner_a(step):
        return high * 8 + lax.rem(low + step, 8)

    def partner_b(step):
        return lax.rem(high + step, n_high) * 8 + low

    def in_copy(pair, block):
        where = (pl.ds(block * GB, GB), pl.ds(pair * 2, 2))
        return pltpu.make_async_copy(
            edge_hbm.at[where], a_buf.at[where], in_sem.at[pair * blocks + block]
        )

    def out_copy(pair, block):
        where = (pl.ds(block * GB, GB), pl.ds(pair * 2, 2))
        return pltpu.make_async_copy(
            a_buf.at[where], edge_out.at[where], out_sem.at[pair * blocks + block]
        )

    def halo_copy(layer, face):
        source, target = ((tx0, rx0), (tx1, rx1))[layer]
        return pltpu.make_async_remote_copy(
            src_ref=source.at[face],
            dst_ref=target.at[face],
            send_sem=h_send.at[layer, face],
            recv_sem=h_recv.at[layer, face],
            device_id=(ahead(offsets[face]),),
            device_id_type=MESH,
        )

    def return_copy(layer, face, distance):
        return pltpu.make_async_remote_copy(
            src_ref=ret_tx.at[layer, face],
            dst_ref=ret_rx.at[layer, face],
            send_sem=r_send.at[layer, face],
            recv_sem=r_recv.at[layer, face],
            device_id=(ahead(distance),),
            device_id_type=MESH,
        )

    def stat_copy(layer, kind, step):
        target, send, recv, partner = (
            (st_a, a_send, a_recv, partner_a),
            (st_b, b_send, b_recv, partner_b),
        )[kind]
        return pltpu.make_async_remote_copy(
            src_ref=st_tx.at[layer, kind],
            dst_ref=target.at[layer, step - 1],
            send_sem=send.at[layer, step - 1],
            recv_sem=recv.at[layer, step - 1],
            device_id=(partner(step),),
            device_id_type=MESH,
        )

    barrier = pltpu.get_barrier_semaphore()
    greeted = [ahead(d) for d in offsets]
    greeted += [partner_a(d) for d in range(1, 8)]
    greeted += [partner_b(d) for d in range(1, n_high)]
    for device in greeted:
        pl.semaphore_signal(barrier, inc=1, device_id=(device,), device_id_type=MESH)

    @pl.loop(0, PAIRS * blocks)
    def _(step):
        in_copy(lax.div(step, blocks), lax.rem(step, blocks)).start()

    @pl.loop(0, nodes // ROWS)
    def _(step):
        rows = pl.ds(step * ROWS, ROWS)
        hb[rows, :] = node_ref[rows, :]
        rowsrc[rows, :] = node_ref[rows, :].astype(F32)

    def gather_rows():
        for face in range(FACES):

            @pl.loop(0, H // 16)
            def _(step):
                for lane in range(16):
                    slot = step * 16 + lane
                    row = rowsrc[pl.ds(send_smem[0, face, slot], 1), :]
                    stage[pl.ds(face * H + slot, 1), :] = row

    gather_rows()
    for face in range(FACES):
        tx0[face] = stage[face * H : (face + 1) * H, :].astype(BF16)
    pl.semaphore_wait(barrier, len(greeted))
    for face in range(FACES):
        halo_copy(0, face).start()

    for layer in range(LAYERS):
        for part in range(3):
            block = ew1[layer, part * T : (part + 1) * T, :].astype(F32)
            w_t[layer, part] = block.T.astype(BF16)
        second = ew2[layer].astype(F32)
        second = second - jnp.mean(second, axis=1, keepdims=True)
        w_t[layer, 3] = second.T.astype(BF16)
        cols[layer, 0] = columns(eb1[layer : layer + 1, :])
        cols[layer, 1] = columns(eg[layer : layer + 1, :])
        cols[layer, 2] = columns(es[layer : layer + 1, :])

    def own_tables(layer, pair_of_groups, latents):
        for part in range(2):
            both = dot_t(w_t[layer, 1 + part], latents).astype(BF16)
            for half in range(2):
                tab[2 * pair_of_groups + half, :, part * T : (part + 1) * T] = both[
                    :, half * T : (half + 1) * T
                ]

    @pl.loop(0, groups // 2)
    def _(step):
        own_tables(0, step, hb[pl.ds(step * 2 * T, 2 * T), :])

    def stage_one(layer, pair, block):
        face_base = (
            nodes
            + (pair * 2 + lax.broadcasted_iota(jnp.int32, (1, 2 * T), 1) // T) * H
        )
        first, far_s, far_r = [], [], []
        for gg in range(GB):
            group = block * GB + gg
            at = pl.multiple_of((group * FACES + pair * 2) * T, T)
            s = ends_ref[0:1, pl.ds(at, 2 * T)]
            r = ends_ref[1:2, pl.ds(at, 2 * T)]
            mine = owned_ref[0:1, pl.ds(at, 2 * T)]
            r = jnp.where(mine > 0, r, -16384)
            near_s = hot(s - group * T, T)
            near_r = hot(r - group * T, T)
            far_s.append(hot(s - face_base, H))
            far_r.append(hot(r - face_base, H))
            ohr[gg] = near_r
            ohh[gg] = far_r[-1]
            got = dot(tab[group], jnp.concatenate([near_s, near_r], axis=0))
            if layer == 0:
                edges = a_buf[group, pl.ds(pair * 2, 2)].reshape(2 * T, T)
                got = got + dot_t(w_t[layer, 0], edges)
            else:
                got = got + dot(w_t[layer, 0], b_buf[group, pair])
            first.append(got)
        bias = cols[layer, 0]
        for face in range(2):
            lanes = slice(face * T, (face + 1) * T)
            for two in range(GB // 2):
                near = (2 * two, 2 * two + 1)
                rhs = jnp.concatenate(
                    [
                        jnp.concatenate([far_s[gg][:, lanes] for gg in near], axis=1),
                        jnp.concatenate([far_r[gg][:, lanes] for gg in near], axis=1),
                    ],
                    axis=0,
                )
                far = dot(htab[face], rhs)
                for half, gg in enumerate(near):
                    before = (
                        first[gg][:, lanes] + far[:, half * T : (half + 1) * T] + bias
                    )
                    hid[gg, :, lanes] = jnp.maximum(before, 0.0).astype(BF16)

    def stage_two(layer, pair, block):
        gain = jnp.concatenate([cols[layer, 1]] * 2, axis=1)
        shift = jnp.concatenate([cols[layer, 2]] * 2, axis=1)
        news = []
        for gg in range(GB):
            group = block * GB + gg
            at = pl.multiple_of((group * FACES + pair * 2) * T, T)
            mine = owned_ref[0:1, pl.ds(at, 2 * T)].astype(F32)
            mixed = dot(w_t[layer, 3], hid[gg])
            spread = jnp.mean(mixed * mixed, axis=0, keepdims=True)
            scale = lax.rsqrt(spread + 1e-05) * mine
            if layer == 0:
                old = a_buf[group, pl.ds(pair * 2, 2)].reshape(2 * T, T).T.astype(F32)
            else:
                old = b_buf[group, pair].astype(F32)
            new = (old + (mixed * scale) * gain + shift * mine).astype(BF16)
            if layer == 0:
                b_buf[group, pair] = new
            else:
                a_buf[group, pl.ds(pair * 2, 2)] = new.T.reshape(2, T, T)
            news.append(new)
            rows = pl.ds(group * T, T)
            agg[rows, :] += dot_t(ohr[gg], new)
        for face in range(2):
            lanes = slice(face * T, (face + 1) * T)
            total = None
            for two in range(GB // 2):
                near = (2 * two, 2 * two + 1)
                part = dot_t(
                    jnp.concatenate([ohh[gg][:, lanes] for gg in near], axis=1),
                    jnp.concatenate([news[gg][:, lanes] for gg in near], axis=1),
                )
                total = part if total is None else total + part
            hsum[face] += total

    def edge_layer(layer, norm):
        @pl.loop(0, nodes // ROWS)
        def _(step):
            agg[pl.ds(step * ROWS, ROWS), :] = jnp.zeros((ROWS, T), F32)

        for pair in range(PAIRS):
            for face in range(2):
                which = 2 * pair + face
                halo_copy(layer, which).wait_recv()
                if layer == 0:
                    rows = rx0[which]
                else:
                    mu, mult, shift = norm
                    update = rx1[which, 0:H, :].astype(F32)
                    update = update + rx1[which, H : H + 1, :].astype(F32)
                    rows = rx0[which].astype(F32) + (update - mu) * mult + shift
                    rows = rows.astype(BF16)
                for part in range(2):
                    htab[face, :, part * H : (part + 1) * H] = dot_t(
                        w_t[layer, 1 + part], rows
                    ).astype(BF16)
            hsum[...] = jnp.zeros_like(hsum)
            if layer == 0:
                in_copy(pair, 0).wait()
            stage_one(layer, pair, 0)

            @pl.loop(1, blocks)
            def _(block):
                if layer == 0:
                    in_copy(pair, block).wait()
                stage_two(layer, pair, block - 1)
                stage_one(layer, pair, block)
                if layer == 1:
                    out_copy(pair, block - 1).start()

            stage_two(layer, pair, blocks - 1)
            if layer == 1:
                out_copy(pair, blocks - 1).start()
            for face in range(2):
                which = 2 * pair + face
                ret_tx[layer, which] = hsum[face].astype(BF16)
            for face in range(2):
                which = 2 * pair + face
                return_copy(layer, which, n_dev - offsets[which]).start()

    def node_layer(layer):
        for face in range(FACES):
            return_copy(layer, face, n_dev - offsets[face]).wait_recv()

        def step_of(step, carry):
            sums, squares = carry
            rows = pl.ds(step * ROWS, ROWS)
            extra = None
            for face in range(FACES):
                picks = hot(send_ref[0, face : face + 1, :] - step * ROWS, ROWS)
                part = dot(picks, ret_rx[layer, face])
                extra = part if extra is None else extra + part
            total = (agg[rows, :] + extra).astype(BF16)
            joined = jnp.concatenate([hb[rows, :], total], axis=1)
            hidden = dot(joined, nw1[layer]) + nb1[layer : layer + 1, :]
            hidden = jnp.maximum(hidden, 0.0).astype(BF16)
            update = dot(hidden, nw2[layer])
            rowsrc[rows, :] = update
            cut = update.reshape(ROWS // 8, 8, T)
            return sums + jnp.sum(cut, axis=0), squares + jnp.sum(cut * cut, axis=0)

        zero = jnp.zeros((8, T), F32)
        sums, squares = lax.fori_loop(0, nodes // ROWS, step_of, (zero, zero))
        sums = jnp.sum(sums, axis=0, keepdims=True)
        squares = jnp.sum(squares, axis=0, keepdims=True)
        first = lax.broadcasted_iota(jnp.int32, (8, T), 0) == 0
        return sums, jnp.where(first, sums, squares)

    def reduce_start(layer, mine):
        st_tx[layer, 0] = mine
        for step in range(1, 8):
            stat_copy(layer, 0, step).start()

    def reduce_finish(layer, mine):
        for step in range(1, 8):
            stat_copy(layer, 0, step).wait_recv()
        for step in range(1, 8):
            mine = mine + st_a[layer, step - 1]
        st_tx[layer, 1] = mine
        for step in range(1, n_high):
            stat_copy(layer, 1, step).start()
        for step in range(1, n_high):
            stat_copy(layer, 1, step).wait_recv()
        for step in range(1, n_high):
            mine = mine + st_b[layer, step - 1]
        count = nodes * n_dev
        mu = mine[0:1, :] / count
        var = jnp.maximum(mine[1:2, :] / count - mu * mu, 0.0)
        mult = ng[layer : layer + 1, :] * lax.rsqrt(var + 1e-05)
        return mu, mult, ns[layer : layer + 1, :]

    edge_layer(0, None)
    sums, mine = node_layer(0)
    reduce_start(0, mine)
    gather_rows()
    ref = (sums / nodes).astype(BF16)
    ref_wide = ref.astype(F32)
    for face in range(FACES):
        delta = stage[face * H : (face + 1) * H, :] - ref_wide
        tx1[face, 0:H, :] = delta.astype(BF16)
        tx1[face, H : H + REF, :] = jnp.broadcast_to(ref_wide, (REF, T)).astype(BF16)
    for face in range(FACES):
        halo_copy(1, face).start()
    mu, mult, shift = reduce_finish(0, mine)

    @pl.loop(0, groups // 2)
    def _(step):
        rows = pl.ds(step * 2 * T, 2 * T)
        new = hb[rows, :].astype(F32) + (rowsrc[rows, :] - mu) * mult + shift
        new = new.astype(BF16)
        hb[rows, :] = new
        own_tables(1, step, new)

    edge_layer(1, (mu, mult, shift))
    _, mine = node_layer(1)
    reduce_start(1, mine)
    mu, mult, shift = reduce_finish(1, mine)

    @pl.loop(0, nodes // ROWS)
    def _(step):
        rows = pl.ds(step * ROWS, ROWS)
        new = hb[rows, :].astype(F32) + (rowsrc[rows, :] - mu) * mult + shift
        node_out[rows, :] = new.astype(BF16)

    @pl.loop(0, PAIRS * blocks)
    def _(step):
        out_copy(lax.div(step, blocks), lax.rem(step, blocks)).wait()

    for layer in range(LAYERS):
        for face in range(FACES):
            halo_copy(layer, face).wait_send()
            return_copy(layer, face, n_dev - offsets[face]).wait_send()
        for step in range(1, 8):
            stat_copy(layer, 0, step).wait_send()
        for step in range(1, n_high):
            stat_copy(layer, 1, step).wait_send()


def per_device(
    n_dev,
    node_latent,
    edge_latent,
    edge_ends,
    edge_owned,
    send_index,
    *weights,
):
    nodes = node_latent.shape[0]
    groups = nodes // T
    slots = edge_latent.shape[0]
    vmem = pl.BlockSpec(memory_space=pltpu.VMEM)
    smem = pl.BlockSpec(memory_space=pltpu.SMEM)
    anywhere = pl.BlockSpec(memory_space=pl.ANY)
    n_copies = PAIRS * (groups // GB)
    n_high = n_dev // 8
    dma = pltpu.SemaphoreType.DMA
    node_out, edge_out = pl.pallas_call(
        functools.partial(kernel, n_dev, groups),
        out_shape=(
            jax.ShapeDtypeStruct((nodes, T), BF16),
            jax.ShapeDtypeStruct((groups, FACES, T, T), BF16),
        ),
        in_specs=[vmem, anywhere, vmem, vmem, smem, vmem] + [vmem] * len(weights),
        out_specs=(vmem, anywhere),
        scratch_shapes=[
            pltpu.VMEM((groups, FACES, T, T), BF16),
            pltpu.VMEM((groups, PAIRS, T, 2 * T), BF16),
            pltpu.VMEM((nodes, T), BF16),
            pltpu.VMEM((nodes, T), F32),
            pltpu.VMEM((nodes, T), F32),
            pltpu.VMEM((groups, T, 2 * T), BF16),
            pltpu.VMEM((2, T, 2 * H), BF16),
            pltpu.VMEM((GB, T, 2 * T), BF16),
            pltpu.VMEM((GB, T, 2 * T), BF16),
            pltpu.VMEM((GB, H, 2 * T), BF16),
            pltpu.VMEM((2, H, T), F32),
            pltpu.VMEM((FACES * H, T), F32),
            pltpu.VMEM((FACES, H, T), BF16),
            pltpu.VMEM((FACES, H + REF, T), BF16),
            pltpu.VMEM((FACES, H, T), BF16),
            pltpu.VMEM((FACES, H + REF, T), BF16),
            pltpu.VMEM((LAYERS, FACES, H, T), BF16),
            pltpu.VMEM((LAYERS, FACES, H, T), BF16),
            pltpu.VMEM((LAYERS, 4, T, T), BF16),
            pltpu.VMEM((LAYERS, 3, T, T), F32),
            pltpu.VMEM((LAYERS, 2, 8, T), F32),
            pltpu.VMEM((LAYERS, 7, 8, T), F32),
            pltpu.VMEM((LAYERS, n_high - 1, 8, T), F32),
            dma((n_copies,)),
            dma((n_copies,)),
            dma((LAYERS, FACES)),
            dma((LAYERS, FACES)),
            dma((LAYERS, FACES)),
            dma((LAYERS, FACES)),
            dma((LAYERS, 7)),
            dma((LAYERS, 7)),
            dma((LAYERS, n_high - 1)),
            dma((LAYERS, n_high - 1)),
        ],
        compiler_params=pltpu.CompilerParams(
            collective_id=0, has_side_effects=True, vmem_limit_bytes=60 * 1024 * 1024
        ),
    )(
        node_latent,
        edge_latent.reshape(groups, FACES, T, T),
        edge_ends,
        edge_owned.reshape(1, slots),
        send_index,
        send_index,
        *weights,
    )
    return node_out, edge_out.reshape(slots, T)


def solution(mesh):
    return jax.shard_map(
        functools.partial(per_device, mesh.shape["blk"]),
        mesh=mesh,
        in_specs=(
            P("blk", None),
            P("blk", None),
            P(None, "blk"),
            P("blk"),
            P("blk", None, None),
        )
        + (P(),) * 10,
        out_specs=(P("blk", None), P("blk", None)),
        check_vma=False,
    )
```

```python
import functools

import jax
import jax.numpy as jnp
from jax import lax
from jax.experimental import pallas as pl
from jax.experimental.pallas import tpu as pltpu
from jax.sharding import PartitionSpec as P

MESH = pl.DeviceIdType.MESH
F32 = jnp.float32
BF16 = jnp.bfloat16
LAYERS = 2
FACES = 6
PAIRS = 3
ORDER = (2, 1, 0)
T = 128
H = 256
SEQUENCE = tuple(2 * pair + face for pair in ORDER for face in range(2))
GB = 4
REF = 16
PART, PARTS = 256, 4
ROWS = 512


def dot(a, b):
    return jnp.dot(a, b, preferred_element_type=F32)


def dot_t(a, b):
    return lax.dot_general(a, b, (((1,), (1,)), ((), ())), preferred_element_type=F32)


def columns(row):
    return jnp.broadcast_to(row, (T, T)).T


def hot(index, rows):
    lanes = index.shape[1]
    code = jnp.broadcast_to(index, (16, lanes)).astype(jnp.int16)
    line = lax.broadcasted_iota(jnp.int32, (rows, lanes), 0).astype(jnp.int16)
    same = line.reshape(rows // 16, 16, lanes) == code[None]
    return jnp.where(same, jnp.ones((), BF16), jnp.zeros((), BF16)).reshape(rows, lanes)


def kernel(
    n_dev,
    groups,
    node_ref,
    edge_hbm,
    ends_ref,
    owned_ref,
    send_smem,
    send_ref,
    ew1,
    eb1,
    ew2,
    eg,
    es,
    nw1,
    nb1,
    nw2,
    ng,
    ns,
    node_out,
    edge_out,
    a_buf,
    b_buf,
    hb,
    rowsrc,
    agg,
    tab,
    htab,
    hid,
    near_hot,
    far_hot,
    hsum,
    stage,
    tx0,
    tx1,
    rx0,
    rx1,
    ret_tx,
    ret_rx,
    w_t,
    cols,
    st_tx,
    st_a,
    st_b,
    in_sem,
    out_sem,
    h_send,
    h_recv,
    r_send,
    r_recv,
    a_send,
    a_recv,
    b_send,
    b_recv,
):
    me = lax.axis_index("blk")
    nodes = groups * T
    blocks = groups // GB
    low, high = lax.rem(me, 8), lax.div(me, 8)
    n_high = n_dev // 8
    offsets = (1, n_dev - 1, 4, n_dev - 4, 16, n_dev - 16)

    def ahead(distance):
        return lax.rem(me + distance, n_dev)

    def partner_a(step):
        return high * 8 + lax.rem(low + step, 8)

    def partner_b(step):
        return lax.rem(high + step, n_high) * 8 + low

    def in_copy(pair, block):
        where = (pl.ds(block * GB, GB), pl.ds(pair * 2, 2))
        return pltpu.make_async_copy(
            edge_hbm.at[where], a_buf.at[where], in_sem.at[pair * blocks + block]
        )

    def out_copy(pair, block):
        where = (pl.ds(block * GB, GB), pl.ds(pair * 2, 2))
        return pltpu.make_async_copy(
            a_buf.at[where], edge_out.at[where], out_sem.at[pair * blocks + block]
        )

    def halo_copy(layer, face):
        source, target = ((tx0, rx0), (tx1, rx1))[layer]
        return pltpu.make_async_remote_copy(
            src_ref=source.at[face],
            dst_ref=target.at[face],
            send_sem=h_send.at[layer, face],
            recv_sem=h_recv.at[layer, face],
            device_id=(ahead(offsets[face]),),
            device_id_type=MESH,
        )

    def return_copy(layer, face, distance):
        return pltpu.make_async_remote_copy(
            src_ref=ret_tx.at[layer, face],
            dst_ref=ret_rx.at[layer, face],
            send_sem=r_send.at[layer, face],
            recv_sem=r_recv.at[layer, face],
            device_id=(ahead(distance),),
            device_id_type=MESH,
        )

    def stat_copy(layer, kind, step):
        target, send, recv, partner = (
            (st_a, a_send, a_recv, partner_a),
            (st_b, b_send, b_recv, partner_b),
        )[kind]
        return pltpu.make_async_remote_copy(
            src_ref=st_tx.at[layer, kind],
            dst_ref=target.at[layer, step - 1],
            send_sem=send.at[layer, step - 1],
            recv_sem=recv.at[layer, step - 1],
            device_id=(partner(step),),
            device_id_type=MESH,
        )

    barrier = pltpu.get_barrier_semaphore()
    greeted = [ahead(d) for d in offsets]
    greeted += [partner_a(d) for d in range(1, 8)]
    greeted += [partner_b(d) for d in range(1, n_high)]
    for device in greeted:
        pl.semaphore_signal(barrier, inc=1, device_id=(device,), device_id_type=MESH)

    @pl.loop(0, PAIRS * blocks)
    def _(step):
        in_copy(lax.div(step, blocks), lax.rem(step, blocks)).start()

    @pl.loop(0, nodes // ROWS)
    def _(step):
        rows = pl.ds(step * ROWS, ROWS)
        hb[rows, :] = node_ref[rows, :]
        rowsrc[rows, :] = node_ref[rows, :].astype(F32)

    def gather_rows():
        @pl.loop(0, FACES)
        def _(face):
            for slot in range(H):
                row = rowsrc[pl.ds(send_smem[face, 0, slot], 1), :]
                stage[pl.ds(face * H + slot, 1), :] = row

    gather_rows()
    for face in range(FACES):
        tx0[face] = stage[face * H : (face + 1) * H, :].astype(BF16)
    pl.semaphore_wait(barrier, len(greeted))
    for face in SEQUENCE:
        halo_copy(0, face).start()

    for layer in range(LAYERS):
        for part in range(3):
            block = ew1[layer, part * T : (part + 1) * T, :].astype(F32)
            w_t[layer, part] = block.T.astype(BF16)
        second = ew2[layer].astype(F32)
        second = second - jnp.mean(second, axis=1, keepdims=True)
        w_t[layer, 3] = second.T.astype(BF16)
        cols[layer, 0] = columns(eb1[layer : layer + 1, :])
        cols[layer, 1] = columns(eg[layer : layer + 1, :])
        cols[layer, 2] = columns(es[layer : layer + 1, :])

    def both_ways(layer):
        return w_t[layer, 1:3].reshape(2 * T, T)

    def own_tables(layer, pair_of_groups, latents):
        both = dot_t(both_ways(layer), latents).astype(BF16)
        for half in range(2):
            for part in range(2):
                tab[2 * pair_of_groups + half, :, part * T : (part + 1) * T] = both[
                    part * T : (part + 1) * T, half * T : (half + 1) * T
                ]

    @pl.loop(0, groups // 2, unroll=4)
    def _(step):
        own_tables(0, step, hb[pl.ds(step * 2 * T, 2 * T), :])

    def ends_of(pair, group):
        at = pl.multiple_of((group * FACES + pair * 2) * T, T)
        lanes = pl.ds(at, 2 * T)
        return ends_ref[0:1, lanes], ends_ref[1:2, lanes], owned_ref[0:1, lanes]

    @pl.loop(0, blocks)
    def _(block):
        for pair in ORDER:
            which = lax.broadcasted_iota(jnp.int32, (1, 2 * T), 1) // T
            face_base = nodes + (pair * 2 + which) * H
            for gg in range(GB):
                group = block * GB + gg
                s, r, mine = ends_of(pair, group)
                far = hot(jnp.where(r >= nodes, r, s) - face_base, H)
                for face in range(2):
                    far_hot[2 * pair + face, block, :, gg * T : (gg + 1) * T] = far[
                        :, face * T : (face + 1) * T
                    ]
                near_hot[group, pair, 0:T, :] = hot(s - group * T, T)
                r = jnp.where(mine > 0, r, -16384)
                near_hot[group, pair, T : 2 * T, :] = hot(r - group * T, T)

    def gather(layer, pair, block):
        first, far = [], []
        for gg in range(GB):
            group = block * GB + gg
            got = dot(tab[group], near_hot[group, pair])
            if layer == 0:
                edges = a_buf[group, pl.ds(pair * 2, 2)].reshape(2 * T, T)
                got = got + dot_t(w_t[layer, 0], edges)
            else:
                got = got + dot(w_t[layer, 0], b_buf[group, pair])
            first.append(got)
        for face in range(2):
            for two in range(GB // 2):
                at = slice(two * 2 * T, (two + 1) * 2 * T)
                far.append(dot(htab[2 * pair + face], far_hot[2 * pair + face, block, :, at]))
        return first, far

    def hide(layer, pair, block, gathered):
        first, far = gathered
        bias = cols[layer, 0]
        for face in range(2):
            lanes = slice(face * T, (face + 1) * T)
            for gg in range(GB):
                remote = ends_of(pair, block * GB + gg)[0][:, lanes] >= nodes
                mask = jnp.broadcast_to(remote, (T, T))
                both = far[face * (GB // 2) + gg // 2]
                side = slice(gg % 2 * T, (gg % 2 + 1) * T)
                add = jnp.where(mask, both[0:T, side], both[T : 2 * T, side])
                before = first[gg][:, lanes] + bias + add
                hid[gg, :, lanes] = jnp.maximum(before, 0.0).astype(BF16)

    def mix(layer):
        return [dot(w_t[layer, 3], hid[gg]) for gg in range(GB)]

    def renew(layer, pair, block, mixes):
        gain = jnp.concatenate([cols[layer, 1]] * 2, axis=1)
        shift = jnp.concatenate([cols[layer, 2]] * 2, axis=1)
        news = []
        for gg in range(GB):
            group = block * GB + gg
            mixed = mixes[gg]
            mine = ends_of(pair, group)[2].astype(F32)
            spread = jnp.mean(mixed * mixed, axis=0, keepdims=True)
            scale = lax.rsqrt(spread + 1e-05) * mine
            if layer == 0:
                old = a_buf[group, pl.ds(pair * 2, 2)].reshape(2 * T, T).T.astype(F32)
            else:
                old = b_buf[group, pair].astype(F32)
            new = (old + (mixed * scale) * gain + shift * mine).astype(BF16)
            if layer == 0:
                b_buf[group, pair] = new
            else:
                a_buf[group, pl.ds(pair * 2, 2)] = new.T.reshape(2, T, T)
            news.append(new)
        return news

    def scatter(pair, block, news):
        sent = []
        for gg in range(GB):
            group = block * GB + gg
            rows = pl.ds(group * T, T)
            agg[rows, :] += dot_t(near_hot[group, pair, T : 2 * T, :], news[gg])
            _, r, mine = ends_of(pair, group)
            leaves = jnp.where((r >= nodes) & (mine > 0), 1.0, 0.0)
            wide = jnp.broadcast_to(leaves, (16, 2 * T)).astype(BF16)
            kept = news[gg].reshape(T // 16, 16, 2 * T) * wide[None]
            sent.append(kept.reshape(T, 2 * T))
        for face in range(2):
            lanes = slice(face * T, (face + 1) * T)
            message = jnp.concatenate([part[:, lanes] for part in sent], axis=1)
            hsum[2 * pair + face] += dot_t(far_hot[2 * pair + face, block], message)

    def edge_layer(layer, norm):
        @pl.loop(0, nodes // ROWS)
        def _(step):
            agg[pl.ds(step * ROWS, ROWS), :] = jnp.zeros((ROWS, T), F32)

        hsum[...] = jnp.zeros_like(hsum)

        def halo_tables(pair):
            faces = (2 * pair, 2 * pair + 1)
            for which in faces:
                halo_copy(layer, which).wait_recv()
            if layer == 0:
                in_copy(pair, 0).wait()
            for which in faces:
                if layer == 0:
                    rows = rx0[which]
                else:
                    mu, mult, shift = norm
                    update = rx1[which, 0:H, :].astype(F32)
                    update = update + rx1[which, H : H + 1, :].astype(F32)
                    rows = rx0[which].astype(F32) + (update - mu) * mult + shift
                    rows = rows.astype(BF16)
                htab[which] = dot_t(both_ways(layer), rows).astype(BF16)

        def turn(pair, block, pair_next, block_next):
            mixes = mix(layer)
            gathered = gather(layer, pair_next, block_next)
            news = renew(layer, pair, block, mixes)
            scatter(pair, block, news)
            hide(layer, pair_next, block_next, gathered)

        halo_tables(ORDER[0])
        hide(layer, ORDER[0], 0, gather(layer, ORDER[0], 0))
        for place, pair in enumerate(ORDER):

            @pl.loop(0, blocks // 2 - 1)
            def _(double):
                block = 2 * double
                if layer == 0:
                    in_copy(pair, block + 1).wait()
                    in_copy(pair, block + 2).wait()
                turn(pair, block, pair, block + 1)
                turn(pair, block + 1, pair, block + 2)
                if layer == 1:
                    out_copy(pair, block).start()
                    out_copy(pair, block + 1).start()

            last = blocks - 1
            if layer == 0:
                in_copy(pair, last).wait()
            if place + 1 < PAIRS:
                halo_tables(ORDER[place + 1])
                turn(pair, last - 1, pair, last)
                turn(pair, last, ORDER[place + 1], 0)
            else:
                turn(pair, last - 1, pair, last)
                scatter(pair, last, renew(layer, pair, last, mix(layer)))
            if layer == 1:
                out_copy(pair, last - 1).start()
                out_copy(pair, last).start()
            for which in (2 * pair, 2 * pair + 1):
                ret_tx[layer, which] = hsum[which].astype(BF16)
            for which in (2 * pair, 2 * pair + 1):
                return_copy(layer, which, n_dev - offsets[which]).start()

    def returned(layer, faces, start, rows):
        extra = agg[pl.ds(start, rows), :]
        for face in faces:
            picks = hot(send_ref[face] - start, rows)
            extra = extra + dot(picks, ret_rx[layer, face])
        return extra

    def node_layer(layer):
        early, late = SEQUENCE[:4], SEQUENCE[4:]
        for face in early:
            return_copy(layer, face, n_dev - offsets[face]).wait_recv()

        @pl.loop(0, nodes // ROWS, unroll=2)
        def _(step):
            agg[pl.ds(step * ROWS, ROWS), :] = returned(layer, early, step * ROWS, ROWS)

        for face in late:
            return_copy(layer, face, n_dev - offsets[face]).wait_recv()

        def step_of(step, carry):
            sums, squares = carry
            starts = [step * (PARTS * PART) + part * PART for part in range(PARTS)]
            totals = [returned(layer, late, at, PART).astype(BF16) for at in starts]
            hiddens = []
            for at, total in zip(starts, totals):
                joined = jnp.concatenate([hb[pl.ds(at, PART), :], total], axis=1)
                hidden = dot(joined, nw1[layer]) + nb1[layer : layer + 1, :]
                hiddens.append(jnp.maximum(hidden, 0.0).astype(BF16))
            for at, hidden in zip(starts, hiddens):
                update = dot(hidden, nw2[layer])
                rowsrc[pl.ds(at, PART), :] = update
                cut = update.reshape(PART // 8, 8, T)
                sums = sums + jnp.sum(cut, axis=0)
                squares = squares + jnp.sum(cut * cut, axis=0)
            return sums, squares

        zero = jnp.zeros((8, T), F32)
        sums, squares = lax.fori_loop(
            0, nodes // (PARTS * PART), step_of, (zero, zero)
        )
        sums = jnp.sum(sums, axis=0, keepdims=True)
        squares = jnp.sum(squares, axis=0, keepdims=True)
        first = lax.broadcasted_iota(jnp.int32, (8, T), 0) == 0
        return sums, jnp.where(first, sums, squares)

    def reduce_start(layer, mine):
        st_tx[layer, 0] = mine
        for step in range(1, 8):
            stat_copy(layer, 0, step).start()

    def reduce_finish(layer, mine):
        for step in range(1, 8):
            stat_copy(layer, 0, step).wait_recv()
        for step in range(1, 8):
            mine = mine + st_a[layer, step - 1]
        st_tx[layer, 1] = mine
        for step in range(1, n_high):
            stat_copy(layer, 1, step).start()
        for step in range(1, n_high):
            stat_copy(layer, 1, step).wait_recv()
        for step in range(1, n_high):
            mine = mine + st_b[layer, step - 1]
        count = nodes * n_dev
        mu = mine[0:1, :] / count
        var = jnp.maximum(mine[1:2, :] / count - mu * mu, 0.0)
        mult = ng[layer : layer + 1, :] * lax.rsqrt(var + 1e-05)
        return mu, mult, ns[layer : layer + 1, :]

    edge_layer(0, None)
    sums, mine = node_layer(0)
    reduce_start(0, mine)
    gather_rows()
    ref = (sums / nodes).astype(BF16)
    ref_wide = ref.astype(F32)
    for face in range(FACES):
        delta = stage[face * H : (face + 1) * H, :] - ref_wide
        tx1[face, 0:H, :] = delta.astype(BF16)
        tx1[face, H : H + REF, :] = jnp.broadcast_to(ref_wide, (REF, T)).astype(BF16)
    for face in SEQUENCE:
        halo_copy(1, face).start()
    mu, mult, shift = reduce_finish(0, mine)

    @pl.loop(0, groups // 2, unroll=4)
    def _(step):
        rows = pl.ds(step * 2 * T, 2 * T)
        new = hb[rows, :].astype(F32) + (rowsrc[rows, :] - mu) * mult + shift
        new = new.astype(BF16)
        hb[rows, :] = new
        own_tables(1, step, new)

    edge_layer(1, (mu, mult, shift))
    _, mine = node_layer(1)
    reduce_start(1, mine)
    mu, mult, shift = reduce_finish(1, mine)

    @pl.loop(0, nodes // ROWS)
    def _(step):
        rows = pl.ds(step * ROWS, ROWS)
        new = hb[rows, :].astype(F32) + (rowsrc[rows, :] - mu) * mult + shift
        node_out[rows, :] = new.astype(BF16)

    @pl.loop(0, PAIRS * blocks)
    def _(step):
        out_copy(lax.div(step, blocks), lax.rem(step, blocks)).wait()

    for layer in range(LAYERS):
        for face in range(FACES):
            halo_copy(layer, face).wait_send()
            return_copy(layer, face, n_dev - offsets[face]).wait_send()
        for step in range(1, 8):
            stat_copy(layer, 0, step).wait_send()
        for step in range(1, n_high):
            stat_copy(layer, 1, step).wait_send()


def per_device(
    n_dev,
    node_latent,
    edge_latent,
    edge_ends,
    edge_owned,
    send_index,
    *weights,
):
    nodes = node_latent.shape[0]
    groups = nodes // T
    slots = edge_latent.shape[0]
    vmem = pl.BlockSpec(memory_space=pltpu.VMEM)
    smem = pl.BlockSpec(memory_space=pltpu.SMEM)
    anywhere = pl.BlockSpec(memory_space=pl.ANY)
    n_copies = PAIRS * (groups // GB)
    n_high = n_dev // 8
    dma = pltpu.SemaphoreType.DMA
    node_out, edge_out = pl.pallas_call(
        functools.partial(kernel, n_dev, groups),
        out_shape=(
            jax.ShapeDtypeStruct((nodes, T), BF16),
            jax.ShapeDtypeStruct((groups, FACES, T, T), BF16),
        ),
        in_specs=[vmem, anywhere, vmem, vmem, smem, vmem] + [vmem] * len(weights),
        out_specs=(vmem, anywhere),
        scratch_shapes=[
            pltpu.VMEM((groups, FACES, T, T), BF16),
            pltpu.VMEM((groups, PAIRS, T, 2 * T), BF16),
            pltpu.VMEM((nodes, T), BF16),
            pltpu.VMEM((nodes, T), F32),
            pltpu.VMEM((nodes, T), F32),
            pltpu.VMEM((groups, T, 2 * T), BF16),
            pltpu.VMEM((FACES, 2 * T, H), BF16),
            pltpu.VMEM((GB, T, 2 * T), BF16),
            pltpu.VMEM((groups, PAIRS, 2 * T, 2 * T), BF16),
            pltpu.VMEM((FACES, groups // GB, H, GB * T), BF16),
            pltpu.VMEM((FACES, H, T), F32),
            pltpu.VMEM((FACES * H, T), F32),
            pltpu.VMEM((FACES, H, T), BF16),
            pltpu.VMEM((FACES, H + REF, T), BF16),
            pltpu.VMEM((FACES, H, T), BF16),
            pltpu.VMEM((FACES, H + REF, T), BF16),
            pltpu.VMEM((LAYERS, FACES, H, T), BF16),
            pltpu.VMEM((LAYERS, FACES, H, T), BF16),
            pltpu.VMEM((LAYERS, 4, T, T), BF16),
            pltpu.VMEM((LAYERS, 3, T, T), F32),
            pltpu.VMEM((LAYERS, 2, 8, T), F32),
            pltpu.VMEM((LAYERS, 7, 8, T), F32),
            pltpu.VMEM((LAYERS, n_high - 1, 8, T), F32),
            dma((n_copies,)),
            dma((n_copies,)),
            dma((LAYERS, FACES)),
            dma((LAYERS, FACES)),
            dma((LAYERS, FACES)),
            dma((LAYERS, FACES)),
            dma((LAYERS, 7)),
            dma((LAYERS, 7)),
            dma((LAYERS, n_high - 1)),
            dma((LAYERS, n_high - 1)),
        ],
        compiler_params=pltpu.CompilerParams(
            collective_id=0, has_side_effects=True, vmem_limit_bytes=56 * 1024 * 1024
        ),
    )(
        node_latent,
        edge_latent.reshape(groups, FACES, T, T),
        edge_ends,
        edge_owned.reshape(1, slots),
        send_index.reshape(FACES, 1, H),
        send_index.reshape(FACES, 1, H),
        *weights,
    )
    return node_out, edge_out.reshape(slots, T)


def solution(mesh):
    return jax.shard_map(
        functools.partial(per_device, mesh.shape["blk"]),
        mesh=mesh,
        in_specs=(
            P("blk", None),
            P("blk", None),
            P(None, "blk"),
            P("blk"),
            P("blk", None, None),
        )
        + (P(),) * 10,
        out_specs=(P("blk", None), P("blk", None)),
        check_vma=False,
    )
```

```python
import functools

import jax
import jax.numpy as jnp
from jax import lax
from jax.experimental import pallas as pl
from jax.experimental.pallas import tpu as pltpu
from jax.sharding import PartitionSpec as P

MESH = pl.DeviceIdType.MESH
F32 = jnp.float32
BF16 = jnp.bfloat16
LAYERS = 2
FACES = 6
PAIRS = 3
ORDER = (2, 1, 0)
T = 128
H = 256
SEQUENCE = tuple(2 * pair + face for pair in ORDER for face in range(2))
GB = 4
REF = 16
PART, PARTS = 256, 4
ROWS = 512


def dot(a, b):
    return jnp.dot(a, b, preferred_element_type=F32)


def dot_t(a, b):
    return lax.dot_general(a, b, (((1,), (1,)), ((), ())), preferred_element_type=F32)


def columns(row):
    return jnp.broadcast_to(row, (T, T)).T


def hot(index, rows):
    lanes = index.shape[1]
    code = jnp.broadcast_to(index, (16, lanes)).astype(jnp.int16)
    line = lax.broadcasted_iota(jnp.int32, (rows, lanes), 0).astype(jnp.int16)
    same = line.reshape(rows // 16, 16, lanes) == code[None]
    return jnp.where(same, jnp.ones((), BF16), jnp.zeros((), BF16)).reshape(rows, lanes)


def kernel(
    n_dev,
    groups,
    node_ref,
    edge_hbm,
    ends_ref,
    owned_ref,
    send_smem,
    send_ref,
    ew1,
    eb1,
    ew2,
    eg,
    es,
    nw1,
    nb1,
    nw2,
    ng,
    ns,
    node_out,
    edge_out,
    a_buf,
    b_buf,
    hb,
    rowsrc,
    agg,
    tab,
    htab,
    hid,
    near_hot,
    far_hot,
    hsum,
    stage,
    tx0,
    tx1,
    rx0,
    rx1,
    ret_tx,
    ret_rx,
    w_t,
    cols,
    st_tx,
    st_a,
    st_b,
    in_sem,
    out_sem,
    h_send,
    h_recv,
    r_send,
    r_recv,
    a_send,
    a_recv,
    b_send,
    b_recv,
    node_sem,
):
    me = lax.axis_index("blk")
    nodes = groups * T
    blocks = groups // GB
    low, high = lax.rem(me, 8), lax.div(me, 8)
    n_high = n_dev // 8
    offsets = (1, n_dev - 1, 4, n_dev - 4, 16, n_dev - 16)

    def ahead(distance):
        return lax.rem(me + distance, n_dev)

    def partner_a(step):
        return high * 8 + lax.rem(low + step, 8)

    def partner_b(step):
        return lax.rem(high + step, n_high) * 8 + low

    def in_copy(pair, block):
        where = (pl.ds(block * GB, GB), pl.ds(pair * 2, 2))
        return pltpu.make_async_copy(
            edge_hbm.at[where], a_buf.at[where], in_sem.at[pair * blocks + block]
        )

    def out_copy(pair, block):
        where = (pl.ds(block * GB, GB), pl.ds(pair * 2, 2))
        return pltpu.make_async_copy(
            a_buf.at[where], edge_out.at[where], out_sem.at[pair * blocks + block]
        )

    def halo_copy(layer, face):
        source, target = ((tx0, rx0), (tx1, rx1))[layer]
        return pltpu.make_async_remote_copy(
            src_ref=source.at[face],
            dst_ref=target.at[face],
            send_sem=h_send.at[layer, face],
            recv_sem=h_recv.at[layer, face],
            device_id=(ahead(offsets[face]),),
            device_id_type=MESH,
        )

    def return_copy(layer, face, distance):
        return pltpu.make_async_remote_copy(
            src_ref=ret_tx.at[layer, face],
            dst_ref=ret_rx.at[layer, face],
            send_sem=r_send.at[layer, face],
            recv_sem=r_recv.at[layer, face],
            device_id=(ahead(distance),),
            device_id_type=MESH,
        )

    def stat_copy(layer, kind, step):
        target, send, recv, partner = (
            (st_a, a_send, a_recv, partner_a),
            (st_b, b_send, b_recv, partner_b),
        )[kind]
        return pltpu.make_async_remote_copy(
            src_ref=st_tx.at[layer, kind],
            dst_ref=target.at[layer, step - 1],
            send_sem=send.at[layer, step - 1],
            recv_sem=recv.at[layer, step - 1],
            device_id=(partner(step),),
            device_id_type=MESH,
        )

    barrier = pltpu.get_barrier_semaphore()
    greeted = [ahead(d) for d in offsets]
    greeted += [partner_a(d) for d in range(1, 8)]
    greeted += [partner_b(d) for d in range(1, n_high)]
    for device in greeted:
        pl.semaphore_signal(barrier, inc=1, device_id=(device,), device_id_type=MESH)

    @pl.loop(0, PAIRS * blocks)
    def _(step):
        in_copy(lax.div(step, blocks), lax.rem(step, blocks)).start()

    @pl.loop(0, nodes // ROWS)
    def _(step):
        rows = pl.ds(step * ROWS, ROWS)
        hb[rows, :] = node_ref[rows, :]
        rowsrc[rows, :] = node_ref[rows, :].astype(F32)

    def gather_rows():
        @pl.loop(0, FACES)
        def _(face):
            for slot in range(H):
                row = rowsrc[pl.ds(send_smem[face, 0, slot], 1), :]
                stage[pl.ds(face * H + slot, 1), :] = row

    gather_rows()
    for face in range(FACES):
        tx0[face] = stage[face * H : (face + 1) * H, :].astype(BF16)
    pl.semaphore_wait(barrier, len(greeted))
    for face in SEQUENCE:
        halo_copy(0, face).start()

    for layer in range(LAYERS):
        for part in range(3):
            block = ew1[layer, part * T : (part + 1) * T, :].astype(F32)
            w_t[layer, part] = block.T.astype(BF16)
        second = ew2[layer].astype(F32)
        second = second - jnp.mean(second, axis=1, keepdims=True)
        w_t[layer, 3] = second.T.astype(BF16)
        cols[layer, 0] = columns(eb1[layer : layer + 1, :])
        cols[layer, 1] = columns(eg[layer : layer + 1, :])
        cols[layer, 2] = columns(es[layer : layer + 1, :])

    def both_ways(layer):
        return w_t[layer, 1:3].reshape(2 * T, T)

    def own_tables(layer, pair_of_groups, latents):
        both = dot_t(both_ways(layer), latents).astype(BF16)
        for half in range(2):
            for part in range(2):
                tab[2 * pair_of_groups + half, :, part * T : (part + 1) * T] = both[
                    part * T : (part + 1) * T, half * T : (half + 1) * T
                ]

    @pl.loop(0, groups // 2, unroll=4)
    def _(step):
        own_tables(0, step, hb[pl.ds(step * 2 * T, 2 * T), :])

    def ends_of(pair, group):
        at = pl.multiple_of((group * FACES + pair * 2) * T, T)
        lanes = pl.ds(at, 2 * T)
        return ends_ref[0:1, lanes], ends_ref[1:2, lanes], owned_ref[0:1, lanes]

    @pl.loop(0, blocks)
    def _(block):
        for pair in ORDER:
            which = lax.broadcasted_iota(jnp.int32, (1, 2 * T), 1) // T
            face_base = nodes + (pair * 2 + which) * H
            for gg in range(GB):
                group = block * GB + gg
                s, r, mine = ends_of(pair, group)
                far = hot(jnp.where(r >= nodes, r, s) - face_base, H)
                for face in range(2):
                    far_hot[2 * pair + face, block, :, gg * T : (gg + 1) * T] = far[
                        :, face * T : (face + 1) * T
                    ]
                near_hot[group, pair, 0:T, :] = hot(s - group * T, T)
                r = jnp.where(mine > 0, r, -16384)
                near_hot[group, pair, T : 2 * T, :] = hot(r - group * T, T)

    def gather(layer, pair, block):
        first, far = [], []
        for gg in range(GB):
            group = block * GB + gg
            got = dot(tab[group], near_hot[group, pair])
            if layer == 0:
                edges = a_buf[group, pl.ds(pair * 2, 2)].reshape(2 * T, T)
                got = got + dot_t(w_t[layer, 0], edges)
            else:
                got = got + dot(w_t[layer, 0], b_buf[group, pair])
            first.append(got)
        for face in range(2):
            for two in range(GB // 2):
                at = slice(two * 2 * T, (two + 1) * 2 * T)
                far.append(dot(htab[2 * pair + face], far_hot[2 * pair + face, block, :, at]))
        return first, far

    def hide(layer, pair, block, gathered):
        first, far = gathered
        bias = cols[layer, 0]
        for face in range(2):
            lanes = slice(face * T, (face + 1) * T)
            for gg in range(GB):
                remote = ends_of(pair, block * GB + gg)[0][:, lanes] >= nodes
                mask = jnp.broadcast_to(remote, (T, T))
                both = far[face * (GB // 2) + gg // 2]
                side = slice(gg % 2 * T, (gg % 2 + 1) * T)
                add = jnp.where(mask, both[0:T, side], both[T : 2 * T, side])
                before = first[gg][:, lanes] + bias + add
                hid[gg, :, lanes] = jnp.maximum(before, 0.0).astype(BF16)

    def mix(layer):
        return [dot(w_t[layer, 3], hid[gg]) for gg in range(GB)]

    def renew(layer, pair, block, mixes):
        gain = jnp.concatenate([cols[layer, 1]] * 2, axis=1)
        shift = jnp.concatenate([cols[layer, 2]] * 2, axis=1)
        news = []
        for gg in range(GB):
            group = block * GB + gg
            mixed = mixes[gg]
            mine = ends_of(pair, group)[2].astype(F32)
            spread = jnp.mean(mixed * mixed, axis=0, keepdims=True)
            scale = lax.rsqrt(spread + 1e-05) * mine
            if layer == 0:
                old = a_buf[group, pl.ds(pair * 2, 2)].reshape(2 * T, T).T.astype(F32)
            else:
                old = b_buf[group, pair].astype(F32)
            new = (old + (mixed * scale) * gain + shift * mine).astype(BF16)
            if layer == 0:
                b_buf[group, pair] = new
            else:
                a_buf[group, pl.ds(pair * 2, 2)] = new.T.reshape(2, T, T)
            news.append(new)
        return news

    def scatter(pair, block, news):
        sent = []
        for gg in range(GB):
            group = block * GB + gg
            rows = pl.ds(group * T, T)
            agg[rows, :] += dot_t(near_hot[group, pair, T : 2 * T, :], news[gg])
            _, r, mine = ends_of(pair, group)
            leaves = jnp.where((r >= nodes) & (mine > 0), 1.0, 0.0)
            wide = jnp.broadcast_to(leaves, (16, 2 * T)).astype(BF16)
            kept = news[gg].reshape(T // 16, 16, 2 * T) * wide[None]
            sent.append(kept.reshape(T, 2 * T))
        for face in range(2):
            lanes = slice(face * T, (face + 1) * T)
            message = jnp.concatenate([part[:, lanes] for part in sent], axis=1)
            hsum[2 * pair + face] += dot_t(far_hot[2 * pair + face, block], message)

    def edge_layer(layer, norm):
        @pl.loop(0, nodes // ROWS)
        def _(step):
            agg[pl.ds(step * ROWS, ROWS), :] = jnp.zeros((ROWS, T), F32)

        hsum[...] = jnp.zeros_like(hsum)

        def halo_tables(pair):
            faces = (2 * pair, 2 * pair + 1)
            for which in faces:
                halo_copy(layer, which).wait_recv()
            if layer == 0:
                in_copy(pair, 0).wait()
            for which in faces:
                if layer == 0:
                    rows = rx0[which]
                else:
                    mu, mult, shift = norm
                    update = rx1[which, 0:H, :].astype(F32)
                    update = update + rx1[which, H : H + 1, :].astype(F32)
                    rows = rx0[which].astype(F32) + (update - mu) * mult + shift
                    rows = rows.astype(BF16)
                htab[which] = dot_t(both_ways(layer), rows).astype(BF16)

        def turn(pair, block, pair_next, block_next):
            mixes = mix(layer)
            gathered = gather(layer, pair_next, block_next)
            news = renew(layer, pair, block, mixes)
            scatter(pair, block, news)
            hide(layer, pair_next, block_next, gathered)

        halo_tables(ORDER[0])
        hide(layer, ORDER[0], 0, gather(layer, ORDER[0], 0))
        for place, pair in enumerate(ORDER):

            @pl.loop(0, blocks // 2 - 1)
            def _(double):
                block = 2 * double
                if layer == 0:
                    in_copy(pair, block + 1).wait()
                    in_copy(pair, block + 2).wait()
                turn(pair, block, pair, block + 1)
                turn(pair, block + 1, pair, block + 2)
                if layer == 1:
                    out_copy(pair, block).start()
                    out_copy(pair, block + 1).start()

            last = blocks - 1
            if layer == 0:
                in_copy(pair, last).wait()
            if place + 1 < PAIRS:
                halo_tables(ORDER[place + 1])
                turn(pair, last - 1, pair, last)
                turn(pair, last, ORDER[place + 1], 0)
            else:
                turn(pair, last - 1, pair, last)
                scatter(pair, last, renew(layer, pair, last, mix(layer)))
            if layer == 1:
                out_copy(pair, last - 1).start()
                out_copy(pair, last).start()
            for which in (2 * pair, 2 * pair + 1):
                ret_tx[layer, which] = hsum[which].astype(BF16)
            for which in (2 * pair, 2 * pair + 1):
                return_copy(layer, which, n_dev - offsets[which]).start()

    def returned(layer, faces, start, rows):
        extra = agg[pl.ds(start, rows), :]
        for face in faces:
            picks = hot(send_ref[face] - start, rows)
            extra = extra + dot(picks, ret_rx[layer, face])
        return extra

    def node_layer(layer):
        early, late = SEQUENCE[:4], SEQUENCE[4:]
        for face in early:
            return_copy(layer, face, n_dev - offsets[face]).wait_recv()

        @pl.loop(0, nodes // ROWS, unroll=2)
        def _(step):
            agg[pl.ds(step * ROWS, ROWS), :] = returned(layer, early, step * ROWS, ROWS)

        for face in late:
            return_copy(layer, face, n_dev - offsets[face]).wait_recv()

        def step_of(step, carry):
            sums, squares = carry
            starts = [step * (PARTS * PART) + part * PART for part in range(PARTS)]
            totals = [returned(layer, late, at, PART).astype(BF16) for at in starts]
            hiddens = []
            for at, total in zip(starts, totals):
                joined = jnp.concatenate([hb[pl.ds(at, PART), :], total], axis=1)
                hidden = dot(joined, nw1[layer]) + nb1[layer : layer + 1, :]
                hiddens.append(jnp.maximum(hidden, 0.0).astype(BF16))
            for at, hidden in zip(starts, hiddens):
                update = dot(hidden, nw2[layer])
                rowsrc[pl.ds(at, PART), :] = update
                cut = update.reshape(PART // 8, 8, T)
                sums = sums + jnp.sum(cut, axis=0)
                squares = squares + jnp.sum(cut * cut, axis=0)
            return sums, squares

        zero = jnp.zeros((8, T), F32)
        sums, squares = lax.fori_loop(
            0, nodes // (PARTS * PART), step_of, (zero, zero)
        )
        sums = jnp.sum(sums, axis=0, keepdims=True)
        squares = jnp.sum(squares, axis=0, keepdims=True)
        first = lax.broadcasted_iota(jnp.int32, (8, T), 0) == 0
        return sums, jnp.where(first, sums, squares)

    def reduce_start(layer, mine):
        st_tx[layer, 0] = mine
        for step in range(1, 8):
            stat_copy(layer, 0, step).start()

    def reduce_finish(layer, mine):
        for step in range(1, 8):
            stat_copy(layer, 0, step).wait_recv()
        for step in range(1, 8):
            mine = mine + st_a[layer, step - 1]
        st_tx[layer, 1] = mine
        for step in range(1, n_high):
            stat_copy(layer, 1, step).start()
        for step in range(1, n_high):
            stat_copy(layer, 1, step).wait_recv()
        for step in range(1, n_high):
            mine = mine + st_b[layer, step - 1]
        count = nodes * n_dev
        mu = mine[0:1, :] / count
        var = jnp.maximum(mine[1:2, :] / count - mu * mu, 0.0)
        mult = ng[layer : layer + 1, :] * lax.rsqrt(var + 1e-05)
        return mu, mult, ns[layer : layer + 1, :]

    edge_layer(0, None)
    sums, mine = node_layer(0)
    reduce_start(0, mine)
    gather_rows()
    ref = (sums / nodes).astype(BF16)
    ref_wide = ref.astype(F32)
    for face in range(FACES):
        delta = stage[face * H : (face + 1) * H, :] - ref_wide
        tx1[face, 0:H, :] = delta.astype(BF16)
        tx1[face, H : H + REF, :] = jnp.broadcast_to(ref_wide, (REF, T)).astype(BF16)
    for face in SEQUENCE:
        halo_copy(1, face).start()
    mu, mult, shift = reduce_finish(0, mine)

    @pl.loop(0, groups // 2, unroll=4)
    def _(step):
        rows = pl.ds(step * 2 * T, 2 * T)
        new = hb[rows, :].astype(F32) + (rowsrc[rows, :] - mu) * mult + shift
        new = new.astype(BF16)
        hb[rows, :] = new
        own_tables(1, step, new)

    edge_layer(1, (mu, mult, shift))
    _, mine = node_layer(1)
    reduce_start(1, mine)
    mu, mult, shift = reduce_finish(1, mine)

    @pl.loop(0, nodes // ROWS)
    def _(step):
        rows = pl.ds(step * ROWS, ROWS)
        new = hb[rows, :].astype(F32) + (rowsrc[rows, :] - mu) * mult + shift
        hb[rows, :] = new.astype(BF16)

    node_copy = pltpu.make_async_copy(hb, node_out, node_sem)
    node_copy.start()

    @pl.loop(0, PAIRS * blocks)
    def _(step):
        out_copy(lax.div(step, blocks), lax.rem(step, blocks)).wait()

    for layer in range(LAYERS):
        for face in range(FACES):
            halo_copy(layer, face).wait_send()
            return_copy(layer, face, n_dev - offsets[face]).wait_send()
        for step in range(1, 8):
            stat_copy(layer, 0, step).wait_send()
        for step in range(1, n_high):
            stat_copy(layer, 1, step).wait_send()

    node_copy.wait()


def per_device(
    n_dev,
    node_latent,
    edge_latent,
    edge_ends,
    edge_owned,
    send_index,
    *weights,
):
    nodes = node_latent.shape[0]
    groups = nodes // T
    slots = edge_latent.shape[0]
    vmem = pl.BlockSpec(memory_space=pltpu.VMEM)
    smem = pl.BlockSpec(memory_space=pltpu.SMEM)
    anywhere = pl.BlockSpec(memory_space=pl.ANY)
    n_copies = PAIRS * (groups // GB)
    n_high = n_dev // 8
    dma = pltpu.SemaphoreType.DMA
    node_out, edge_out = pl.pallas_call(
        functools.partial(kernel, n_dev, groups),
        out_shape=(
            pltpu.VMEM((nodes, T), BF16),
            pltpu.VMEM((groups, FACES, T, T), BF16),
        ),
        in_specs=[vmem, anywhere, vmem, vmem, smem, vmem] + [vmem] * len(weights),
        out_specs=(anywhere, anywhere),
        scratch_shapes=[
            pltpu.VMEM((groups, FACES, T, T), BF16),
            pltpu.VMEM((groups, PAIRS, T, 2 * T), BF16),
            pltpu.VMEM((nodes, T), BF16),
            pltpu.VMEM((nodes, T), F32),
            pltpu.VMEM((nodes, T), F32),
            pltpu.VMEM((groups, T, 2 * T), BF16),
            pltpu.VMEM((FACES, 2 * T, H), BF16),
            pltpu.VMEM((GB, T, 2 * T), BF16),
            pltpu.VMEM((groups, PAIRS, 2 * T, 2 * T), BF16),
            pltpu.VMEM((FACES, groups // GB, H, GB * T), BF16),
            pltpu.VMEM((FACES, H, T), F32),
            pltpu.VMEM((FACES * H, T), F32),
            pltpu.VMEM((FACES, H, T), BF16),
            pltpu.VMEM((FACES, H + REF, T), BF16),
            pltpu.VMEM((FACES, H, T), BF16),
            pltpu.VMEM((FACES, H + REF, T), BF16),
            pltpu.VMEM((LAYERS, FACES, H, T), BF16),
            pltpu.VMEM((LAYERS, FACES, H, T), BF16),
            pltpu.VMEM((LAYERS, 4, T, T), BF16),
            pltpu.VMEM((LAYERS, 3, T, T), F32),
            pltpu.VMEM((LAYERS, 2, 8, T), F32),
            pltpu.VMEM((LAYERS, 7, 8, T), F32),
            pltpu.VMEM((LAYERS, n_high - 1, 8, T), F32),
            dma((n_copies,)),
            dma((n_copies,)),
            dma((LAYERS, FACES)),
            dma((LAYERS, FACES)),
            dma((LAYERS, FACES)),
            dma((LAYERS, FACES)),
            dma((LAYERS, 7)),
            dma((LAYERS, 7)),
            dma((LAYERS, n_high - 1)),
            dma((LAYERS, n_high - 1)),
            dma,
        ],
        compiler_params=pltpu.CompilerParams(
            collective_id=0, has_side_effects=True, vmem_limit_bytes=56 * 1024 * 1024
        ),
    )(
        node_latent,
        edge_latent.reshape(groups, FACES, T, T),
        edge_ends,
        edge_owned.reshape(1, slots),
        send_index.reshape(FACES, 1, H),
        send_index.reshape(FACES, 1, H),
        *weights,
    )
    return node_out, edge_out.reshape(slots, T)


def solution(mesh):
    return jax.shard_map(
        functools.partial(per_device, mesh.shape["blk"]),
        mesh=mesh,
        in_specs=(
            P("blk", None),
            P("blk", None),
            P(None, "blk"),
            P("blk"),
            P("blk", None, None),
        )
        + (P(),) * 10,
        out_specs=(P("blk", None), P("blk", None)),
        check_vma=False,
    )
```

```python
import functools

import jax
import jax.numpy as jnp
from jax import lax
from jax.experimental import pallas as pl
from jax.experimental.pallas import tpu as pltpu
from jax.sharding import PartitionSpec as P

MESH = pl.DeviceIdType.MESH
F32 = jnp.float32
BF16 = jnp.bfloat16
LAYERS = 2
FACES = 6
PAIRS = 3
ORDER = (2, 1, 0)
T = 128
H = 256
SEQUENCE = tuple(2 * pair + face for pair in ORDER for face in range(2))
GB = 4
REF = 16
PART, PARTS = 256, 4
ROWS = 512


def dot(a, b):
    return jnp.dot(a, b, preferred_element_type=F32)


def dot_t(a, b):
    return lax.dot_general(a, b, (((1,), (1,)), ((), ())), preferred_element_type=F32)


def columns(row):
    return jnp.broadcast_to(row, (T, T)).T


def hot(index, rows):
    lanes = index.shape[1]
    code = jnp.broadcast_to(index, (16, lanes)).astype(jnp.int16)
    line = lax.broadcasted_iota(jnp.int32, (rows, lanes), 0).astype(jnp.int16)
    same = line.reshape(rows // 16, 16, lanes) == code[None]
    return jnp.where(same, jnp.ones((), BF16), jnp.zeros((), BF16)).reshape(rows, lanes)


def kernel(
    n_dev,
    groups,
    node_ref,
    edge_hbm,
    ends_ref,
    owned_ref,
    send_smem,
    send_ref,
    ew1,
    eb1,
    ew2,
    eg,
    es,
    nw1,
    nb1,
    nw2,
    ng,
    ns,
    node_out,
    edge_out,
    a_buf,
    b_buf,
    hb,
    rowsrc,
    agg,
    tab,
    htab,
    hid,
    near_hot,
    far_hot,
    hsum,
    stage,
    tx0,
    tx1,
    rx0,
    rx1,
    ret_tx,
    ret_rx,
    w_t,
    cols,
    st_tx,
    st_a,
    st_b,
    in_sem,
    out_sem,
    h_send,
    h_recv,
    r_send,
    r_recv,
    a_send,
    a_recv,
    b_send,
    b_recv,
    node_sem,
):
    me = lax.axis_index("blk")
    nodes = groups * T
    blocks = groups // GB
    low, high = lax.rem(me, 8), lax.div(me, 8)
    n_high = n_dev // 8
    offsets = (1, n_dev - 1, 4, n_dev - 4, 16, n_dev - 16)

    def ahead(distance):
        return lax.rem(me + distance, n_dev)

    def partner_a(step):
        return high * 8 + lax.rem(low + step, 8)

    def partner_b(step):
        return lax.rem(high + step, n_high) * 8 + low

    def in_copy(pair, block):
        where = (pl.ds(block * GB, GB), pl.ds(pair * 2, 2))
        return pltpu.make_async_copy(
            edge_hbm.at[where], a_buf.at[where], in_sem.at[pair * blocks + block]
        )

    def out_copy(pair, block):
        where = (pl.ds(block * GB, GB), pl.ds(pair * 2, 2))
        return pltpu.make_async_copy(
            a_buf.at[where], edge_out.at[where], out_sem.at[pair * blocks + block]
        )

    def halo_copy(layer, face):
        source, target = ((tx0, rx0), (tx1, rx1))[layer]
        return pltpu.make_async_remote_copy(
            src_ref=source.at[face],
            dst_ref=target.at[face],
            send_sem=h_send.at[layer, face],
            recv_sem=h_recv.at[layer, face],
            device_id=(ahead(offsets[face]),),
            device_id_type=MESH,
        )

    def return_copy(layer, face, distance):
        return pltpu.make_async_remote_copy(
            src_ref=ret_tx.at[layer, face],
            dst_ref=ret_rx.at[layer, face],
            send_sem=r_send.at[layer, face],
            recv_sem=r_recv.at[layer, face],
            device_id=(ahead(distance),),
            device_id_type=MESH,
        )

    def stat_copy(layer, kind, step):
        target, send, recv, partner = (
            (st_a, a_send, a_recv, partner_a),
            (st_b, b_send, b_recv, partner_b),
        )[kind]
        return pltpu.make_async_remote_copy(
            src_ref=st_tx.at[layer, kind],
            dst_ref=target.at[layer, step - 1],
            send_sem=send.at[layer, step - 1],
            recv_sem=recv.at[layer, step - 1],
            device_id=(partner(step),),
            device_id_type=MESH,
        )

    barrier = pltpu.get_barrier_semaphore()
    greeted = [ahead(d) for d in offsets]
    greeted += [partner_a(d) for d in range(1, 8)]
    greeted += [partner_b(d) for d in range(1, n_high)]
    for device in greeted:
        pl.semaphore_signal(barrier, inc=1, device_id=(device,), device_id_type=MESH)

    @pl.loop(0, PAIRS * blocks)
    def _(step):
        in_copy(lax.div(step, blocks), lax.rem(step, blocks)).start()

    @pl.loop(0, nodes // ROWS)
    def _(step):
        rows = pl.ds(step * ROWS, ROWS)
        hb[rows, :] = node_ref[rows, :]
        rowsrc[rows, :] = node_ref[rows, :].astype(F32)

    def gather_rows():
        @pl.loop(0, FACES)
        def _(face):
            for slot in range(H):
                row = rowsrc[pl.ds(send_smem[face, 0, slot], 1), :]
                stage[pl.ds(face * H + slot, 1), :] = row

    gather_rows()
    for face in range(FACES):
        tx0[face] = stage[face * H : (face + 1) * H, :].astype(BF16)
    pl.semaphore_wait(barrier, len(greeted))
    for face in SEQUENCE:
        halo_copy(0, face).start()

    for layer in range(LAYERS):
        for part in range(3):
            block = ew1[layer, part * T : (part + 1) * T, :].astype(F32)
            w_t[layer, part] = block.T.astype(BF16)
        second = ew2[layer].astype(F32)
        second = second - jnp.mean(second, axis=1, keepdims=True)
        w_t[layer, 3] = second.T.astype(BF16)
        cols[layer, 0] = columns(eb1[layer : layer + 1, :])
        cols[layer, 1] = columns(eg[layer : layer + 1, :])
        cols[layer, 2] = columns(es[layer : layer + 1, :])

    def both_ways(layer):
        return w_t[layer, 1:3].reshape(2 * T, T)

    def own_tables(layer, pair_of_groups, latents):
        both = dot_t(both_ways(layer), latents).astype(BF16)
        for half in range(2):
            for part in range(2):
                tab[2 * pair_of_groups + half, :, part * T : (part + 1) * T] = both[
                    part * T : (part + 1) * T, half * T : (half + 1) * T
                ]

    @pl.loop(0, groups // 2, unroll=4)
    def _(step):
        own_tables(0, step, hb[pl.ds(step * 2 * T, 2 * T), :])

    def ends_of(pair, group):
        at = pl.multiple_of((group * FACES + pair * 2) * T, T)
        lanes = pl.ds(at, 2 * T)
        return ends_ref[0:1, lanes], ends_ref[1:2, lanes], owned_ref[0:1, lanes]

    @pl.loop(0, blocks)
    def _(block):
        for pair in ORDER:
            which = lax.broadcasted_iota(jnp.int32, (1, 2 * T), 1) // T
            face_base = nodes + (pair * 2 + which) * H
            for gg in range(GB):
                group = block * GB + gg
                s, r, mine = ends_of(pair, group)
                far = hot(jnp.where(r >= nodes, r, s) - face_base, H)
                for face in range(2):
                    far_hot[2 * pair + face, block, :, gg * T : (gg + 1) * T] = far[
                        :, face * T : (face + 1) * T
                    ]
                near_hot[group, pair, 0:T, :] = hot(s - group * T, T)
                r = jnp.where(mine > 0, r, -16384)
                near_hot[group, pair, T : 2 * T, :] = hot(r - group * T, T)

    def gather(layer, pair, block):
        first, far = [], []
        for gg in range(GB):
            group = block * GB + gg
            got = dot(tab[group], near_hot[group, pair])
            if layer == 0:
                edges = a_buf[group, pl.ds(pair * 2, 2)].reshape(2 * T, T)
                got = got + dot_t(w_t[layer, 0], edges)
            else:
                got = got + dot(w_t[layer, 0], b_buf[group, pair])
            first.append(got)
        for face in range(2):
            for two in range(GB // 2):
                at = slice(two * 2 * T, (two + 1) * 2 * T)
                far.append(dot(htab[2 * pair + face], far_hot[2 * pair + face, block, :, at]))
        return first, far

    def hide(layer, pair, block, gathered):
        first, far = gathered
        bias = cols[layer, 0]
        for face in range(2):
            lanes = slice(face * T, (face + 1) * T)
            for gg in range(GB):
                remote = ends_of(pair, block * GB + gg)[0][:, lanes] >= nodes
                mask = jnp.broadcast_to(remote, (T, T))
                both = far[face * (GB // 2) + gg // 2]
                side = slice(gg % 2 * T, (gg % 2 + 1) * T)
                add = jnp.where(mask, both[0:T, side], both[T : 2 * T, side])
                before = first[gg][:, lanes] + bias + add
                hid[gg, :, lanes] = jnp.maximum(before, 0.0).astype(BF16)

    def mix(layer):
        return [dot(w_t[layer, 3], hid[gg]) for gg in range(GB)]

    def renew(layer, pair, block, mixes):
        gain = jnp.concatenate([cols[layer, 1]] * 2, axis=1)
        shift = jnp.concatenate([cols[layer, 2]] * 2, axis=1)
        news = []
        for gg in range(GB):
            group = block * GB + gg
            mixed = mixes[gg]
            mine = ends_of(pair, group)[2].astype(F32)
            spread = jnp.mean(mixed * mixed, axis=0, keepdims=True)
            scale = lax.rsqrt(spread + 1e-05) * mine
            if layer == 0:
                old = a_buf[group, pl.ds(pair * 2, 2)].reshape(2 * T, T).T.astype(F32)
            else:
                old = b_buf[group, pair].astype(F32)
            new = (old + (mixed * scale) * gain + shift * mine).astype(BF16)
            if layer == 0:
                b_buf[group, pair] = new
            else:
                a_buf[group, pl.ds(pair * 2, 2)] = new.T.reshape(2, T, T)
            news.append(new)
        return news

    def scatter(pair, block, news):
        sent = []
        for gg in range(GB):
            group = block * GB + gg
            rows = pl.ds(group * T, T)
            agg[rows, :] += dot_t(near_hot[group, pair, T : 2 * T, :], news[gg])
            _, r, mine = ends_of(pair, group)
            leaves = jnp.where((r >= nodes) & (mine > 0), 1.0, 0.0)
            wide = jnp.broadcast_to(leaves, (16, 2 * T)).astype(BF16)
            kept = news[gg].reshape(T // 16, 16, 2 * T) * wide[None]
            sent.append(kept.reshape(T, 2 * T))
        for face in range(2):
            lanes = slice(face * T, (face + 1) * T)
            message = jnp.concatenate([part[:, lanes] for part in sent], axis=1)
            hsum[2 * pair + face] += dot_t(far_hot[2 * pair + face, block], message)

    def clear():
        @pl.loop(0, nodes // ROWS)
        def _(step):
            agg[pl.ds(step * ROWS, ROWS), :] = jnp.zeros((ROWS, T), F32)

        hsum[...] = jnp.zeros_like(hsum)

    def edge_layer(layer, norm):
        def halo_tables(pair):
            faces = (2 * pair, 2 * pair + 1)
            for which in faces:
                halo_copy(layer, which).wait_recv()
            if layer == 0:
                in_copy(pair, 0).wait()
            for which in faces:
                if layer == 0:
                    rows = rx0[which]
                else:
                    mu, mult, shift = norm
                    update = rx1[which, 0:H, :].astype(F32)
                    update = update + rx1[which, H : H + 1, :].astype(F32)
                    rows = rx0[which].astype(F32) + (update - mu) * mult + shift
                    rows = rows.astype(BF16)
                htab[which] = dot_t(both_ways(layer), rows).astype(BF16)

        def turn(pair, block, pair_next, block_next):
            mixes = mix(layer)
            gathered = gather(layer, pair_next, block_next)
            news = renew(layer, pair, block, mixes)
            scatter(pair, block, news)
            hide(layer, pair_next, block_next, gathered)

        halo_tables(ORDER[0])
        hide(layer, ORDER[0], 0, gather(layer, ORDER[0], 0))
        for place, pair in enumerate(ORDER):

            @pl.loop(0, blocks // 2 - 1)
            def _(double):
                block = 2 * double
                if layer == 0:
                    in_copy(pair, block + 1).wait()
                    in_copy(pair, block + 2).wait()
                turn(pair, block, pair, block + 1)
                turn(pair, block + 1, pair, block + 2)
                if layer == 1:
                    out_copy(pair, block).start()
                    out_copy(pair, block + 1).start()

            last = blocks - 1
            if layer == 0:
                in_copy(pair, last).wait()
            if place + 1 < PAIRS:
                halo_tables(ORDER[place + 1])
                turn(pair, last - 1, pair, last)
                turn(pair, last, ORDER[place + 1], 0)
            else:
                turn(pair, last - 1, pair, last)
                scatter(pair, last, renew(layer, pair, last, mix(layer)))
            if layer == 1:
                out_copy(pair, last - 1).start()
                out_copy(pair, last).start()
            for which in (2 * pair, 2 * pair + 1):
                ret_tx[layer, which] = hsum[which].astype(BF16)
            for which in (2 * pair, 2 * pair + 1):
                return_copy(layer, which, n_dev - offsets[which]).start()

    def returned(layer, faces, start, rows):
        extra = agg[pl.ds(start, rows), :]
        for face in faces:
            picks = hot(send_ref[face] - start, rows)
            extra = extra + dot(picks, ret_rx[layer, face])
        return extra

    def node_layer(layer):
        early, late = SEQUENCE[:4], SEQUENCE[4:]
        for face in early:
            return_copy(layer, face, n_dev - offsets[face]).wait_recv()

        @pl.loop(0, nodes // ROWS, unroll=2)
        def _(step):
            agg[pl.ds(step * ROWS, ROWS), :] = returned(layer, early, step * ROWS, ROWS)

        for face in late:
            return_copy(layer, face, n_dev - offsets[face]).wait_recv()

        def step_of(step, carry):
            sums, squares = carry
            starts = [step * (PARTS * PART) + part * PART for part in range(PARTS)]
            totals = [returned(layer, late, at, PART).astype(BF16) for at in starts]
            hiddens = []
            for at, total in zip(starts, totals):
                joined = jnp.concatenate([hb[pl.ds(at, PART), :], total], axis=1)
                hidden = dot(joined, nw1[layer]) + nb1[layer : layer + 1, :]
                hiddens.append(jnp.maximum(hidden, 0.0).astype(BF16))
            for at, hidden in zip(starts, hiddens):
                update = dot(hidden, nw2[layer])
                rowsrc[pl.ds(at, PART), :] = update
                cut = update.reshape(PART // 8, 8, T)
                sums = sums + jnp.sum(cut, axis=0)
                squares = squares + jnp.sum(cut * cut, axis=0)
            return sums, squares

        zero = jnp.zeros((8, T), F32)
        sums, squares = lax.fori_loop(
            0, nodes // (PARTS * PART), step_of, (zero, zero)
        )
        sums = jnp.sum(sums, axis=0, keepdims=True)
        squares = jnp.sum(squares, axis=0, keepdims=True)
        return sums, jnp.concatenate([sums, squares], axis=0)

    def reduce_start(layer, mine):
        st_tx[layer, 0] = mine
        for step in range(1, 8):
            stat_copy(layer, 0, step).start()

    def sent(layer):
        for face in range(FACES):
            halo_copy(layer, face).wait_send()
            return_copy(layer, face, n_dev - offsets[face]).wait_send()
        for step in range(1, 8):
            stat_copy(layer, 0, step).wait_send()
        if layer == 1:
            for step in range(1, n_high):
                stat_copy(0, 1, step).wait_send()

            @pl.loop(0, PAIRS * blocks)
            def _(step):
                out_copy(lax.div(step, blocks), lax.rem(step, blocks)).wait()

    def reduce_finish(layer, mine, beside):
        for step in range(1, 8):
            stat_copy(layer, 0, step).wait_recv()
        for step in range(1, 8):
            mine = mine + st_a[layer, step - 1]
        st_tx[layer, 1] = mine
        for step in range(1, n_high):
            stat_copy(layer, 1, step).start()
        beside()
        for step in range(1, n_high):
            stat_copy(layer, 1, step).wait_recv()
        for step in range(1, n_high):
            mine = mine + st_b[layer, step - 1]
        count = nodes * n_dev
        mu = mine[0:1, :] / count
        var = jnp.maximum(mine[1:2, :] / count - mu * mu, 0.0)
        mult = ng[layer : layer + 1, :] * lax.rsqrt(var + 1e-05)
        return mu, mult, ns[layer : layer + 1, :]

    clear()
    edge_layer(0, None)
    sums, mine = node_layer(0)
    reduce_start(0, mine)
    gather_rows()
    ref = (sums / nodes).astype(BF16)
    ref_wide = ref.astype(F32)
    for face in range(FACES):
        delta = stage[face * H : (face + 1) * H, :] - ref_wide
        tx1[face, 0:H, :] = delta.astype(BF16)
        tx1[face, H : H + REF, :] = jnp.broadcast_to(ref_wide, (REF, T)).astype(BF16)
    for face in SEQUENCE:
        halo_copy(1, face).start()
    clear()
    mu, mult, shift = reduce_finish(0, mine, functools.partial(sent, 0))

    @pl.loop(0, groups // 2, unroll=4)
    def _(step):
        rows = pl.ds(step * 2 * T, 2 * T)
        new = hb[rows, :].astype(F32) + (rowsrc[rows, :] - mu) * mult + shift
        new = new.astype(BF16)
        hb[rows, :] = new
        own_tables(1, step, new)

    edge_layer(1, (mu, mult, shift))
    _, mine = node_layer(1)
    reduce_start(1, mine)
    mu, mult, shift = reduce_finish(1, mine, functools.partial(sent, 1))

    @pl.loop(0, nodes // ROWS)
    def _(step):
        rows = pl.ds(step * ROWS, ROWS)
        new = hb[rows, :].astype(F32) + (rowsrc[rows, :] - mu) * mult + shift
        hb[rows, :] = new.astype(BF16)

    node_copy = pltpu.make_async_copy(hb, node_out, node_sem)
    node_copy.start()

    for step in range(1, n_high):
        stat_copy(1, 1, step).wait_send()

    node_copy.wait()


def per_device(
    n_dev,
    node_latent,
    edge_latent,
    edge_ends,
    edge_owned,
    send_index,
    *weights,
):
    nodes = node_latent.shape[0]
    groups = nodes // T
    slots = edge_latent.shape[0]
    vmem = pl.BlockSpec(memory_space=pltpu.VMEM)
    smem = pl.BlockSpec(memory_space=pltpu.SMEM)
    anywhere = pl.BlockSpec(memory_space=pl.ANY)
    n_copies = PAIRS * (groups // GB)
    n_high = n_dev // 8
    dma = pltpu.SemaphoreType.DMA
    node_out, edge_out = pl.pallas_call(
        functools.partial(kernel, n_dev, groups),
        out_shape=(
            pltpu.VMEM((nodes, T), BF16),
            pltpu.VMEM((groups, FACES, T, T), BF16),
        ),
        in_specs=[vmem, anywhere, vmem, vmem, smem, vmem] + [vmem] * len(weights),
        out_specs=(anywhere, anywhere),
        scratch_shapes=[
            pltpu.VMEM((groups, FACES, T, T), BF16),
            pltpu.VMEM((groups, PAIRS, T, 2 * T), BF16),
            pltpu.VMEM((nodes, T), BF16),
            pltpu.VMEM((nodes, T), F32),
            pltpu.VMEM((nodes, T), F32),
            pltpu.VMEM((groups, T, 2 * T), BF16),
            pltpu.VMEM((FACES, 2 * T, H), BF16),
            pltpu.VMEM((GB, T, 2 * T), BF16),
            pltpu.VMEM((groups, PAIRS, 2 * T, 2 * T), BF16),
            pltpu.VMEM((FACES, groups // GB, H, GB * T), BF16),
            pltpu.VMEM((FACES, H, T), F32),
            pltpu.VMEM((FACES * H, T), F32),
            pltpu.VMEM((FACES, H, T), BF16),
            pltpu.VMEM((FACES, H + REF, T), BF16),
            pltpu.VMEM((FACES, H, T), BF16),
            pltpu.VMEM((FACES, H + REF, T), BF16),
            pltpu.VMEM((LAYERS, FACES, H, T), BF16),
            pltpu.VMEM((LAYERS, FACES, H, T), BF16),
            pltpu.VMEM((LAYERS, 4, T, T), BF16),
            pltpu.VMEM((LAYERS, 3, T, T), F32),
            pltpu.VMEM((LAYERS, 2, 2, T), F32),
            pltpu.VMEM((LAYERS, 7, 2, T), F32),
            pltpu.VMEM((LAYERS, n_high - 1, 2, T), F32),
            dma((n_copies,)),
            dma((n_copies,)),
            dma((LAYERS, FACES)),
            dma((LAYERS, FACES)),
            dma((LAYERS, FACES)),
            dma((LAYERS, FACES)),
            dma((LAYERS, 7)),
            dma((LAYERS, 7)),
            dma((LAYERS, n_high - 1)),
            dma((LAYERS, n_high - 1)),
            dma,
        ],
        compiler_params=pltpu.CompilerParams(
            collective_id=0, has_side_effects=True, vmem_limit_bytes=56 * 1024 * 1024
        ),
    )(
        node_latent,
        edge_latent.reshape(groups, FACES, T, T),
        edge_ends,
        edge_owned.reshape(1, slots),
        send_index.reshape(FACES, 1, H),
        send_index.reshape(FACES, 1, H),
        *weights,
    )
    return node_out, edge_out.reshape(slots, T)


def solution(mesh):
    return jax.shard_map(
        functools.partial(per_device, mesh.shape["blk"]),
        mesh=mesh,
        in_specs=(
            P("blk", None),
            P("blk", None),
            P(None, "blk"),
            P("blk"),
            P("blk", None, None),
        )
        + (P(),) * 10,
        out_specs=(P("blk", None), P("blk", None)),
        check_vma=False,
    )
```
